32 devices in a mesh: grp: 4 (over y, x), seq: 8 (over z, core).
Axes of the slice: x: 2, y: 2, z: 4, core: 2. Of those that a mesh axis runs over, the one named last changes fastest.
Arguments:
- queries: bfloat16 [8, 256, 8192], P('grp', 'seq'), parts along dimension 0, may hold values from -400 to 400
- stretch_keys: bfloat16 [8, 256, 1024], P('grp', 'seq'), parts along dimension 0, may hold values from -6 to 6
- stretch_values: bfloat16 [8, 256, 1024], P('grp', 'seq'), parts along dimension 0, may hold values from -6 to 6
- cache_keys: bfloat16 [8, 512, 1024], P('grp', 'seq'), parts along dimension 0, may hold values from -6 to 6
- cache_values: bfloat16 [8, 512, 1024], P('grp', 'seq'), parts along dimension 0, may hold values from -6 to 6
- prefix_len: int32 [8], P('grp'), parts along dimension 0, may hold values from 16 to 512, as said below
Outputs:
- attention: bfloat16 [8, 256, 8192], P('grp', 'seq'), parts along dimension 0
- prefix_bounds: bfloat16 [8, 32, 2048], P('grp', 'seq'), parts along dimension 0
- stretch_bounds: bfloat16 [8, 16, 2048], P('grp', 'seq'), parts along dimension 0
The draws below stay inside these ranges and needn't reach their ends.
There are 4 independent parts, one for each index of `grp`. The reference program is written for one: setup_inputs(seed, part) draws one part's arguments, and reference() takes and returns one part's arrays. A program takes and returns all parts, laid end to end along the dimension named above; each array names one. Nothing has to cross between parts.
Inputs may be any that keep to these rules, and one draw needn't show every extreme that they name: `prefix_len`: multiples of 16; some sequence of every group has 512.
All inputs are finite; a program needn't handle non-finite values.
Results may differ from the reference program's by a relative error of at most 0.006.
Values may be sent and summed in bfloat16 or wider, within the bound.
A program may use at most 128 MiB of HBM per device.

```python
import math
import jax
import jax.numpy as jnp
from jax import lax

HQ = 64
HK = 8
DH = 128
PAGE = 16
SEQS = 2
STRETCH = 256
PREFIX = 512


def key_field(base):
    field_values = jnp.clip(jax.random.normal(jax.random.fold_in(base, 11), (SEQS, STRETCH, HK * DH), jnp.float32), -6.0, 6.0)
    return field_values


def draw_stretch_keys(key, part):
    return key_field(key).astype(jnp.bfloat16)


def draw_queries(key, part):
    field_values = jnp.clip(jax.random.normal(jax.random.fold_in(key, 12), (SEQS, STRETCH, HQ * DH), jnp.float32), -6.0, 6.0)
    return field_values.astype(jnp.bfloat16)


def draw_prefix_len(key, part):
    page_count = jax.random.randint(jax.random.fold_in(key, 21), (SEQS,), 1, PREFIX // PAGE + 1)
    full_seq = jax.random.randint(jax.random.fold_in(key, 22), (), 0, SEQS)
    page_count = jnp.where(jnp.arange(SEQS) == full_seq, PREFIX // PAGE, page_count)
    return (page_count * PAGE).astype(jnp.int32)


def steps_of(rng, dims, shards, smallest, high):
    loudness = 1.0
    for dim, blocks in shards:
        steps = jax.random.uniform(jax.random.fold_in(jax.random.fold_in(rng, 6), dim), (blocks,), jnp.float32, smallest / len(shards), high / len(shards))
        loudness = loudness * jnp.repeat(jnp.exp(steps), dims[dim] // blocks).reshape((-1,) + (1,) * (len(dims) - 1 - dim))
    return loudness


def scatter_about(stream_key, extent, spread, most, split=(), kind=jnp.bfloat16):
    factor_of = steps_of(stream_key, extent, split, -0.22, 0.18) if split else 1.0
    array = jax.random.normal(stream_key, extent, jnp.float32) * spread * factor_of
    return jnp.minimum(jnp.maximum(array, -most), most).astype(kind)


def setup_inputs(seed: int = 0, part: int = 0) -> dict:
    keys = jax.random.split(jax.random.key(seed), 7)
    part_splits = jax.random.split(jax.random.fold_in(keys[6], part), 7)
    queries = draw_queries(jax.random.fold_in(jax.random.fold_in(keys[6], part), 71), part)
    stretch_keys = draw_stretch_keys(jax.random.fold_in(jax.random.fold_in(keys[6], part), 71), part)
    stretch_values = scatter_about(part_splits[2], (SEQS, STRETCH, HK * DH), 1.0, 6.0, ((1, 8),))
    cache_keys = scatter_about(part_splits[3], (SEQS, PREFIX, HK * DH), 1.0, 6.0, ((1, 8),))
    cache_values = scatter_about(part_splits[4], (SEQS, PREFIX, HK * DH), 1.0, 6.0, ((1, 8),))
    prefix_len = draw_prefix_len(jax.random.fold_in(jax.random.fold_in(keys[6], part), 71), part)
    return dict(queries=queries, stretch_keys=stretch_keys, stretch_values=stretch_values, cache_keys=cache_keys, cache_values=cache_values, prefix_len=prefix_len)


def page_bounds(key_rows, live_pages):
    shaped = key_rows.reshape(key_rows.shape[0] // PAGE, PAGE, key_rows.shape[1])
    joined = jnp.concatenate([lax.optimization_barrier(jnp.min(shaped, axis=1)), lax.optimization_barrier(jnp.max(shaped, axis=1))], axis=1)
    return jnp.where(live_pages[:, None], joined, jnp.zeros_like(joined))

def reference(queries, stretch_keys, stretch_values, cache_keys, cache_values, prefix_len):
    group = HQ // HK
    factor = 1.0 / math.sqrt(DH)
    block = math.gcd(STRETCH, 256)
    key_index = jnp.arange(PREFIX + STRETCH, dtype=jnp.int32)

    def one_sequence(operands):
        query_rows, new_keys, new_values, old_keys, old_values, length = operands
        key_rows = jnp.concatenate([old_keys, new_keys], axis=0).astype(jnp.float32).reshape(PREFIX + STRETCH, HK, DH)
        value_rows = jnp.concatenate([old_values, new_values], axis=0).astype(jnp.float32).reshape(PREFIX + STRETCH, HK, DH)

        def one_block(offset):
            query_block = lax.dynamic_slice_in_dim(query_rows, offset, block, 0).astype(jnp.float32).reshape(block, HK, group, DH)
            scores = jnp.einsum('rhgd,khd->rhgk', query_block, key_rows) * factor
            row_index = offset + jnp.arange(block, dtype=jnp.int32)
            live = jnp.where(key_index[None, :] < PREFIX, key_index[None, :] < length, key_index[None, :] - PREFIX <= row_index[:, None])
            live = live[:, None, None, :]
            top_score = lax.optimization_barrier(jnp.max(jnp.where(live, scores, -1e+30), axis=-1, keepdims=True))
            weights = jnp.where(live, jnp.exp(scores - top_score), 0.0)
            weight_sum = lax.optimization_barrier(jnp.sum(weights, axis=-1))
            rounded = lax.optimization_barrier(weights.astype(jnp.bfloat16)).astype(jnp.float32)
            mixed = jnp.einsum('rhgk,khd->rhgd', rounded, value_rows) / weight_sum[..., None]
            return mixed.reshape(block, HQ * DH).astype(jnp.bfloat16)
        offsets = jnp.arange(STRETCH // block, dtype=jnp.int32) * block
        attention = lax.map(one_block, offsets).reshape(STRETCH, HQ * DH)
        old_live = jnp.arange(PREFIX // PAGE, dtype=jnp.int32) * PAGE < length
        new_live = jnp.ones((STRETCH // PAGE,), dtype=bool)
        return (attention, page_bounds(old_keys, old_live), page_bounds(new_keys, new_live))
    attention, prefix_bounds, stretch_bounds = lax.map(one_sequence, (queries, stretch_keys, stretch_values, cache_keys, cache_values, prefix_len))
    return (attention, prefix_bounds, stretch_bounds)
```

```python
import functools
import math

import jax
import jax.numpy as jnp
from jax import lax
from jax.experimental import pallas as pl
from jax.experimental.pallas import tpu as pltpu
from jax.sharding import PartitionSpec as P

HQ = 64
HK = 8
DH = 128
PAGE = 16
GROUP = HQ // HK
HALF = HK // 2
WIDE = GROUP * DH
SHIP = 2
MESH = pl.DeviceIdType.MESH
MASKED = -1e30


def kernel(n, q, sk, sv, ck, cv, plen, out, pb, sb, kv, qall, oall, bias, ckv, skv, qsem, lsem, dsend, drecv,
           qmsend, qmrecv, rsend, rrecv, lsend, lrecv, xsend, xrecv, ssend, srecv, oloc, osend, orecv, posend, porecv, bsem):
    seqs, rows, _ = q.shape
    pre = ck.shape[1]
    chips = n // 2
    last = chips - 1
    cache_keys = n * pre
    me = lax.axis_index("seq")
    c, k = me // 2, me % 2
    mate = c * 2 + (1 - k)
    reach = jnp.maximum(c, last - c)

    def remote(src, dst, send, recv, target):
        return pltpu.make_async_remote_copy(
            src_ref=src, dst_ref=dst, send_sem=send, recv_sem=recv, device_id={"seq": target}, device_id_type=MESH)

    sources = ((ck, 0, 0, pre), (cv, 1, 0, pre), (sk, 0, cache_keys, rows), (sv, 1, cache_keys, rows))

    def own_copy(h, i):
        src, which, base, length = sources[i]
        lanes = pl.ds(pl.multiple_of((k * HALF + h) * DH, DH), DH)
        return pltpu.make_async_copy(
            src.at[:, :, lanes], kv.at[h, which, :, pl.ds(base + me * length, length), :], lsem.at[h, i])

    def mate_copy(h, i):
        src, which, base, length = sources[i]
        lanes = pl.ds(pl.multiple_of(((1 - k) * HALF + h) * DH, DH), DH)
        return remote(src.at[:, :, lanes], kv.at[h, which, :, pl.ds(base + me * length, length), :],
                      dsend.at[h, i], drecv.at[h, i], mate)

    def wide_lanes(core, h):
        return pl.ds(pl.multiple_of((core * HALF + h) * WIDE, WIDE), WIDE)

    def own_q(h):
        return pltpu.make_async_copy(q.at[:, :, wide_lanes(k, h)], qall.at[0, h, :, k], qsem.at[h])

    def mate_q(h):
        return remote(q.at[:, :, wide_lanes(1 - k, h)], qall.at[0, h, :, k], qmsend.at[h], qmrecv.at[h], mate)

    def ship_q(h, core, target):
        return remote(q.at[:, :, wide_lanes(core, h)], qall.at[1, h, :, k], xsend.at[h, core], xrecv.at[h, k], target)

    def cache_rows(j):
        return pl.ds(pl.multiple_of(j * 2 * pre, 2 * pre), 2 * pre)

    def stretch_rows(j):
        return pl.ds(pl.multiple_of(cache_keys + j * 2 * rows, 2 * rows), 2 * rows)

    def right_copy(h, j, part):
        where = kv.at[h, :, :, cache_rows(j) if part == 0 else stretch_rows(j), :]
        return remote(where, where, rsend.at[h, j, part], rrecv.at[h, j, part], jnp.minimum(me + 2, n - 1))

    def left_copy(h, j):
        where = kv.at[h, :, :, cache_rows(j), :]
        return remote(where, where, lsend.at[h, j], lrecv.at[h, j], jnp.maximum(me - 2, 0))

    def ship_stretch(h):
        where = kv.at[h, :, :, stretch_rows(last), :]
        return remote(where, where, ssend.at[h], srecv.at[h], jnp.maximum(me - 2, 0))

    def out_own(h):
        return pltpu.make_async_copy(oall.at[0, h, :, k], out.at[:, :, wide_lanes(k, h)], oloc.at[h])

    def out_mate(h):
        return remote(oall.at[0, h, :, 1 - k], out.at[:, :, wide_lanes(k, h)], osend.at[h], orecv.at[h], mate)

    def out_ship(h, dev):
        return remote(oall.at[1, h, :, dev], out.at[:, :, wide_lanes(k, h)], posend.at[h, dev], porecv.at[h, k],
                      last * 2 + dev)

    for h in range(HALF):
        for i in range(4):
            own_copy(h, i).start()
    bound_copies = (pltpu.make_async_copy(ck, ckv, bsem.at[0]), pltpu.make_async_copy(sk, skv, bsem.at[1]))
    for copy in bound_copies:
        copy.start()
    for h in range(HALF):
        own_q(h).start()

    @pl.loop(c + 1, chips)
    def _(j):
        for h in range(HALF):
            kv[h, :, :, stretch_rows(j), :] = jnp.zeros((2, seqs, 2 * rows, DH), jnp.bfloat16)

    barrier = pltpu.get_barrier_semaphore()
    pl.semaphore_signal(barrier, inc=1, device_id={"seq": mate}, device_id_type=MESH)

    @pl.when(c > 0)
    def _():
        for core in range(2):
            pl.semaphore_signal(barrier, inc=1, device_id={"seq": (c - 1) * 2 + core}, device_id_type=MESH)

    @pl.when(c < last)
    def _():
        for core in range(2):
            pl.semaphore_signal(barrier, inc=1, device_id={"seq": (c + 1) * 2 + core}, device_id_type=MESH)

    pl.semaphore_wait(barrier, 1 + 2 * (c > 0).astype(jnp.int32) + 2 * (c < last).astype(jnp.int32))

    for h in range(HALF):
        for i in range(4):
            mate_copy(h, i).start()
    for h in range(HALF):
        @pl.when((c < last) | (h >= SHIP))
        def _():
            mate_q(h).start()

    def bounds_of(keys, s, live):
        pages = keys.shape[1] // PAGE
        block = keys[s].astype(jnp.float32).reshape(pages, PAGE, HK * DH)
        low, high = jnp.min(block, axis=1), jnp.max(block, axis=1)
        if live is not None:
            low, high = jnp.where(live, low, 0.0), jnp.where(live, high, 0.0)
        return low.astype(jnp.bfloat16), high.astype(jnp.bfloat16)

    def local_work():
        token = lax.broadcasted_iota(jnp.int32, (rows, n * rows), 0)
        col = lax.broadcasted_iota(jnp.int32, (rows, n * rows), 1)
        slot = lax.broadcasted_iota(jnp.int32, (rows, cache_keys), 1)
        for s in range(seqs):
            cached = jnp.where(slot < plen[s], 0.0, MASKED)
            for side in range(2):
                first = (c if side == 0 else last) * 2 * rows
                for dev in range(2):
                    bias[side, s, dev, :, :cache_keys] = cached
                    bias[side, s, dev, :, cache_keys:] = jnp.where(col <= token + (first + dev * rows), 0.0, MASKED)
        for copy in bound_copies:
            copy.wait()
        width = HK * DH
        for s in range(seqs):
            page = me * (pre // PAGE) + lax.broadcasted_iota(jnp.int32, (pre // PAGE, width), 0)
            low, high = bounds_of(ckv, s, page * PAGE < plen[s])
            pb[s, :, :width] = low
            pb[s, :, width:] = high
            low, high = bounds_of(skv, s, None)
            sb[s, :, :width] = low
            sb[s, :, width:] = high

    def attend(h, side, s, dev):
        scale = math.log2(math.e) / math.sqrt(DH)
        query = jnp.concatenate([qall[side, h, s, dev, :, g * DH:(g + 1) * DH] for g in range(GROUP)], axis=0)
        scores = lax.dot_general(query, kv[h, 0, s], (((1,), (1,)), ((), ())), preferred_element_type=jnp.float32)
        keys = scores.shape[1]
        scores = scores.reshape(GROUP, rows, keys) + bias[side, s, dev][None]
        scores = scores.reshape(GROUP * rows, keys)
        top = jnp.max(scores, axis=1, keepdims=True)
        weights = jnp.exp2((scores - top) * scale)
        total = jnp.sum(weights, axis=1, keepdims=True)
        mixed = jnp.dot(weights.astype(jnp.bfloat16), kv[h, 1, s], preferred_element_type=jnp.float32)
        mixed = (mixed / total).astype(jnp.bfloat16)
        for g in range(GROUP):
            oall[side, h, s, dev, :, g * DH:(g + 1) * DH] = mixed[g * rows:(g + 1) * rows]

    def shipped(h):
        return h < SHIP

    def from_left(h, d):
        return (c - d >= 0) & jnp.logical_not((c == last) & shipped(h))

    def to_right(h, d):
        return (c < last) & (c - d >= 0) & jnp.logical_not((c + 1 == last) & shipped(h))

    def to_left(h, d):
        return (c > 0) & (c + d <= last)

    def one_slot(t):
        @pl.loop(0, HALF)
        def _(back):
            h = HALF - 1 - back
            d = t - h

            @pl.when((d >= 0) & (d <= last))
            def _():
                @pl.when(d == 0)
                def _():
                    for i in range(4):
                        own_copy(h, i).wait()
                        mate_copy(h, i).wait_recv()

                @pl.when((d > 0) & from_left(h, d))
                def _():
                    for part in range(2):
                        right_copy(h, c - d, part).wait_recv()

                @pl.when(to_right(h, d))
                def _():
                    for part in range(2):
                        right_copy(h, c - d, part).start()

                @pl.when((d > 0) & (c + d <= last))
                def _():
                    left_copy(h, c + d).wait_recv()

                @pl.when(to_left(h, d))
                def _():
                    left_copy(h, c + d).start()

                @pl.when((d == 0) & (c == last) & shipped(h))
                def _():
                    for core in range(2):
                        ship_q(h, core, (last - 1) * 2 + core).start()
                    ship_stretch(h).start()

        h = t - reach
        @pl.when((h >= 0) & (h < HALF) & ((c < last) | jnp.logical_not(shipped(h))))
        def _():
            extra = (c == last - 1) & shipped(h)

            @pl.when(extra)
            def _():
                for core in range(2):
                    remote(q.at[:, :, wide_lanes(core, h)], qall.at[1, h, :, core], xsend.at[h, core],
                           xrecv.at[h, core], mate).wait_recv()
                ship_stretch(h).wait_recv()

            own_q(h).wait()
            remote(q.at[:, :, wide_lanes(k, h)], qall.at[0, h, :, 1 - k], qmsend.at[h], qmrecv.at[h], mate).wait_recv()

            @pl.loop(jnp.where(extra, 0, 2 * seqs), 4 * seqs)
            def _(step):
                mine = step // (2 * seqs)
                rest = step % (2 * seqs)
                attend(h, 1 - mine, rest // 2, rest % 2)

                @pl.when(step == 2 * seqs - 1)
                def _():
                    for dev in range(2):
                        out_ship(h, dev).start()

            out_own(h).start()
            out_mate(h).start()

    one_slot(0)
    local_work()

    @pl.loop(1, HALF + last)
    def _(t):
        one_slot(t)

    @pl.loop(0, HALF)
    def _(h):
        for i in range(4):
            mate_copy(h, i).wait_send()

        @pl.when((c < last) | jnp.logical_not(shipped(h)))
        def _():
            mate_q(h).wait_send()
            out_own(h).wait()
            out_mate(h).wait_send()
            remote(oall.at[0, h, :, k], out.at[:, :, wide_lanes(1 - k, h)], osend.at[h], orecv.at[h], mate).wait_recv()

        @pl.when((c == last) & shipped(h))
        def _():
            own_q(h).wait()
            ship_stretch(h).wait_send()
            for core in range(2):
                ship_q(h, core, (last - 1) * 2 + core).wait_send()
                remote(oall.at[0, h, :, k], out.at[:, :, wide_lanes(core, h)], posend.at[h, core], porecv.at[h, core],
                       mate).wait_recv()

        @pl.when((c == last - 1) & shipped(h))
        def _():
            for dev in range(2):
                out_ship(h, dev).wait_send()

        @pl.loop(0, chips)
        def _(d):
            @pl.when(to_right(h, d))
            def _():
                for part in range(2):
                    right_copy(h, c - d, part).wait_send()

            @pl.when(to_left(h, d))
            def _():
                left_copy(h, c + d).wait_send()


def on_device(n, queries, stretch_keys, stretch_values, cache_keys, cache_values, prefix_len):
    seqs, rows, width = queries.shape
    pre = cache_keys.shape[1]
    chips = n // 2
    keys = n * (pre + rows)
    dma = pltpu.SemaphoreType.DMA
    hbm = pl.BlockSpec(memory_space=pl.ANY)
    vmem = pl.BlockSpec(memory_space=pltpu.VMEM)
    return pl.pallas_call(
        functools.partial(kernel, n),
        out_shape=(
            jax.ShapeDtypeStruct((seqs, rows, width), jnp.bfloat16),
            jax.ShapeDtypeStruct((seqs, pre // PAGE, 2 * HK * DH), jnp.bfloat16),
            jax.ShapeDtypeStruct((seqs, rows // PAGE, 2 * HK * DH), jnp.bfloat16),
        ),
        in_specs=[hbm] * 5 + [pl.BlockSpec(memory_space=pltpu.SMEM)],
        out_specs=(hbm, vmem, vmem),
        scratch_shapes=[
            pltpu.VMEM((HALF, 2, seqs, keys, DH), jnp.bfloat16),
            pltpu.VMEM((2, HALF, seqs, 2, rows, WIDE), jnp.bfloat16),
            pltpu.VMEM((2, HALF, seqs, 2, rows, WIDE), jnp.bfloat16),
            pltpu.VMEM((2, seqs, 2, rows, keys), jnp.float32),
            pltpu.VMEM((seqs, pre, HK * DH), jnp.bfloat16),
            pltpu.VMEM((seqs, rows, HK * DH), jnp.bfloat16),
            dma((HALF,)),
            dma((HALF, 4)),
            dma((HALF, 4)), dma((HALF, 4)),
            dma((HALF,)), dma((HALF,)),
            dma((HALF, chips, 2)), dma((HALF, chips, 2)),
            dma((HALF, chips)), dma((HALF, chips)),
            dma((HALF, 2)), dma((HALF, 2)),
            dma((HALF,)), dma((HALF,)),
            dma((HALF,)),
            dma((HALF,)), dma((HALF,)),
            dma((HALF, 2)), dma((HALF, 2)),
            dma((2,)),
        ],
        compiler_params=pltpu.CompilerParams(
            collective_id=0, has_side_effects=True, vmem_limit_bytes=60 * 1024 * 1024),
    )(queries, stretch_keys, stretch_values, cache_keys, cache_values, prefix_len)


def solution(mesh):
    rows = P("grp", "seq", None)
    return jax.shard_map(
        functools.partial(on_device, mesh.shape["seq"]),
        mesh=mesh,
        in_specs=(rows, rows, rows, rows, rows, P("grp")),
        out_specs=(rows, rows, rows),
        check_vma=False,
    )
```

```python
import functools
import math

import jax
import jax.numpy as jnp
from jax import lax
from jax.experimental import pallas as pl
from jax.experimental.pallas import tpu as pltpu
from jax.sharding import PartitionSpec as P

HQ = 64
HK = 8
DH = 128
PAGE = 16
GROUP = HQ // HK
HALF = HK // 2
WIDE = GROUP * DH
SHIP = 5
LEAD = 1
MESH = pl.DeviceIdType.MESH
MASKED = -1e30


def kernel(n, q, sk, sv, ck, cv, plen, out, pb, sb, kv, qall, oall, bias, ckv, skv, qsem, lsem, dsend, drecv,
           qmsend, qmrecv, rsend, rrecv, lsend, lrecv, xsend, xrecv, ssend, srecv, oloc, osend, orecv, posend, porecv, bsem):
    seqs, rows, _ = q.shape
    pre = ck.shape[1]
    chips = n // 2
    last = chips - 1
    cache_keys = n * pre
    me = lax.axis_index("seq")
    c, k = me // 2, me % 2
    mate = c * 2 + (1 - k)
    units = HALF * seqs
    reach = jnp.maximum(c, last - c)

    def remote(src, dst, send, recv, target):
        return pltpu.make_async_remote_copy(
            src_ref=src, dst_ref=dst, send_sem=send, recv_sem=recv, device_id={"seq": target}, device_id_type=MESH)

    sources = ((ck, 0, 0, pre), (cv, 1, 0, pre), (sk, 0, cache_keys, rows), (sv, 1, cache_keys, rows))

    def place(ref, side, u, dev):
        return ref.at[side, u // seqs, u % seqs, dev]

    def keys_of(u, which, span):
        return kv.at[u // seqs, which, u % seqs, span, :]

    def both_of(u, span):
        return kv.at[u // seqs, :, u % seqs, span, :]

    def lanes_of(core, u):
        return pl.ds(pl.multiple_of((core * HALF + u // seqs) * DH, DH), DH)

    def own_copy(u, i):
        src, which, base, length = sources[i]
        return pltpu.make_async_copy(
            src.at[u % seqs, :, lanes_of(k, u)], keys_of(u, which, pl.ds(base + me * length, length)), lsem.at[u, i])

    def mate_copy(u, i):
        src, which, base, length = sources[i]
        return remote(src.at[u % seqs, :, lanes_of(1 - k, u)], keys_of(u, which, pl.ds(base + me * length, length)),
                      dsend.at[u, i], drecv.at[u, i], mate)

    def wide(ref, core, u):
        return ref.at[u % seqs, :, pl.ds(pl.multiple_of((core * HALF + u // seqs) * WIDE, WIDE), WIDE)]

    def own_q(u):
        return pltpu.make_async_copy(wide(q, k, u), place(qall, 0, u, k), qsem.at[u])

    def mate_q(u, dev):
        return remote(wide(q, 1 - k, u), place(qall, 0, u, dev), qmsend.at[u], qmrecv.at[u], mate)

    def ship_q(u, core, dev):
        return remote(wide(q, core, u), place(qall, 1, u, dev), xsend.at[u, core], xrecv.at[u, dev],
                      jnp.maximum(last - 1, 0) * 2 + core)

    def cache_rows(j):
        return pl.ds(pl.multiple_of(j * 2 * pre, 2 * pre), 2 * pre)

    def stretch_rows(j):
        return pl.ds(pl.multiple_of(cache_keys + j * 2 * rows, 2 * rows), 2 * rows)

    def right_copy(u, j, part):
        where = both_of(u, cache_rows(j) if part == 0 else stretch_rows(j))
        return remote(where, where, rsend.at[u, j, part], rrecv.at[u, j, part], jnp.minimum(me + 2, n - 1))

    def left_copy(u, j):
        where = both_of(u, cache_rows(j))
        return remote(where, where, lsend.at[u, j], lrecv.at[u, j], jnp.maximum(me - 2, 0))

    def ship_stretch(u):
        where = both_of(u, stretch_rows(last))
        return remote(where, where, ssend.at[u], srecv.at[u], jnp.maximum(me - 2, 0))

    def out_own(u):
        return pltpu.make_async_copy(place(oall, 0, u, k), wide(out, k, u), oloc.at[u])

    def out_mate(u, core):
        return remote(place(oall, 0, u, 1 - k), wide(out, core, u), osend.at[u], orecv.at[u], mate)

    def out_ship(u, dev, core):
        return remote(place(oall, 1, u, dev), wide(out, core, u), posend.at[u, dev], porecv.at[u, core],
                      last * 2 + dev)

    for u in range(units):
        for i in range(4):
            own_copy(u, i).start()
    bound_copies = (pltpu.make_async_copy(ck, ckv, bsem.at[0]), pltpu.make_async_copy(sk, skv, bsem.at[1]))
    for u in range(units):
        own_q(u).start()
    for copy in bound_copies:
        copy.start()

    @pl.loop(c + 1, chips)
    def _(j):
        for h in range(HALF):
            kv[h, :, :, stretch_rows(j), :] = jnp.zeros((2, seqs, 2 * rows, DH), jnp.bfloat16)

    barrier = pltpu.get_barrier_semaphore()
    pl.semaphore_signal(barrier, inc=1, device_id={"seq": mate}, device_id_type=MESH)

    @pl.when(c > 0)
    def _():
        for core in range(2):
            pl.semaphore_signal(barrier, inc=1, device_id={"seq": (c - 1) * 2 + core}, device_id_type=MESH)

    @pl.when(c < last)
    def _():
        for core in range(2):
            pl.semaphore_signal(barrier, inc=1, device_id={"seq": (c + 1) * 2 + core}, device_id_type=MESH)

    pl.semaphore_wait(barrier, 1 + 2 * (c > 0).astype(jnp.int32) + 2 * (c < last).astype(jnp.int32))

    for u in range(units):
        for i in range(4):
            mate_copy(u, i).start()
    for u in range(units):
        @pl.when((c < last) | (u < units - SHIP))
        def _():
            mate_q(u, k).start()

    def bounds_of(keys, s, live):
        pages = keys.shape[1] // PAGE
        block = keys[s].astype(jnp.float32).reshape(pages, PAGE, HK * DH)
        low, high = jnp.min(block, axis=1), jnp.max(block, axis=1)
        if live is not None:
            low, high = jnp.where(live, low, 0.0), jnp.where(live, high, 0.0)
        return low.astype(jnp.bfloat16), high.astype(jnp.bfloat16)

    def local_work():
        token = lax.broadcasted_iota(jnp.int32, (rows, n * rows), 0)
        col = lax.broadcasted_iota(jnp.int32, (rows, n * rows), 1)
        slot = lax.broadcasted_iota(jnp.int32, (rows, cache_keys), 1)
        for s in range(seqs):
            cached = jnp.where(slot < plen[s], 0.0, MASKED)
            for side in range(2):
                first = (c if side == 0 else last) * 2 * rows
                for dev in range(2):
                    bias[side, s, dev, :, :cache_keys] = cached
                    bias[side, s, dev, :, cache_keys:] = jnp.where(col <= token + (first + dev * rows), 0.0, MASKED)
        for copy in bound_copies:
            copy.wait()
        width = HK * DH
        for s in range(seqs):
            page = me * (pre // PAGE) + lax.broadcasted_iota(jnp.int32, (pre // PAGE, width), 0)
            low, high = bounds_of(ckv, s, page * PAGE < plen[s])
            pb[s, :, :width] = low
            pb[s, :, width:] = high
            low, high = bounds_of(skv, s, None)
            sb[s, :, :width] = low
            sb[s, :, width:] = high

    def attend(u, side):
        scale = math.log2(math.e) / math.sqrt(DH)
        h, s = u // seqs, u % seqs
        for dev in range(2):
            query = jnp.concatenate([qall[side, h, s, dev, :, g * DH:(g + 1) * DH] for g in range(GROUP)], axis=0)
            scores = lax.dot_general(query, kv[h, 0, s], (((1,), (1,)), ((), ())), preferred_element_type=jnp.float32)
            keys = scores.shape[1]
            scores = scores.reshape(GROUP, rows, keys) + bias[side, s, dev][None]
            scores = scores.reshape(GROUP * rows, keys)
            top = jnp.max(scores, axis=1, keepdims=True)
            weights = jnp.exp2((scores - top) * scale)
            total = jnp.sum(weights, axis=1, keepdims=True)
            mixed = jnp.dot(weights.astype(jnp.bfloat16), kv[h, 1, s], preferred_element_type=jnp.float32)
            mixed = (mixed / total).astype(jnp.bfloat16)
            for g in range(GROUP):
                oall[side, h, s, dev, :, g * DH:(g + 1) * DH] = mixed[g * rows:(g + 1) * rows]

    def shipped(u):
        return u >= units - SHIP

    def from_left(u, d):
        return (c - d >= 0) & jnp.logical_not((c == last) & shipped(u))

    def to_right(u, d):
        return (c < last) & (c - d >= 0) & jnp.logical_not((c + 1 == last) & shipped(u))

    def to_left(u, d):
        return (c > 0) & (c + d <= last)

    def own_ready(u):
        @pl.when(u < units)
        def _():
            for i in range(4):
                own_copy(u, i).wait()
                mate_copy(u, i).wait_recv()

            @pl.when(c < last)
            def _():
                @pl.when(to_right(u, 0))
                def _():
                    for part in range(2):
                        right_copy(u, c, part).start()

            @pl.when(c > 0)
            def _():
                left_copy(u, c).start()

            @pl.when((c == last) & shipped(u))
            def _():
                ship_stretch(u).start()

        given = u + min(LEAD, units - SHIP)

        @pl.when((c == last) & (given < units) & shipped(given))
        def _():
            for core in range(2):
                ship_q(given, core, k).start()

    def one_slot(t):
        own_ready(t)

        @pl.loop(1, chips)
        def _(d):
            u = t - d

            @pl.when((u >= 0) & (u < units))
            def _():
                @pl.when(from_left(u, d))
                def _():
                    for part in range(2):
                        right_copy(u, c - d, part).wait_recv()

                @pl.when(to_right(u, d))
                def _():
                    for part in range(2):
                        right_copy(u, c - d, part).start()

        @pl.loop(1, chips)
        def _(d):
            u = t - d

            @pl.when((u >= 0) & (u < units) & (c + d <= last))
            def _():
                left_copy(u, c + d).wait_recv()

                @pl.when(to_left(u, d))
                def _():
                    left_copy(u, c + d).start()

        u = t - reach

        @pl.when((u >= 0) & (u < units) & ((c < last) | jnp.logical_not(shipped(u))))
        def _():
            extra = (c == last - 1) & shipped(u)

            @pl.when(extra)
            def _():
                for dev in range(2):
                    ship_q(u, k, dev).wait_recv()
                ship_stretch(u).wait_recv()

            own_q(u).wait()
            mate_q(u, 1 - k).wait_recv()

            @pl.loop(jnp.where(extra, 0, 1), 2)
            def _(step):
                attend(u, 1 - step)

                @pl.when(step == 0)
                def _():
                    for dev in range(2):
                        out_ship(u, dev, k).start()

            out_own(u).start()
            out_mate(u, k).start()

    one_slot(0)
    local_work()

    @pl.loop(1, units + last)
    def _(t):
        one_slot(t)

    @pl.loop(0, units)
    def _(u):
        for i in range(4):
            mate_copy(u, i).wait_send()

        @pl.when((c < last) | jnp.logical_not(shipped(u)))
        def _():
            mate_q(u, k).wait_send()
            out_own(u).wait()
            out_mate(u, k).wait_send()
            out_mate(u, 1 - k).wait_recv()

        @pl.when((c == last) & shipped(u))
        def _():
            own_q(u).wait()
            ship_stretch(u).wait_send()
            for core in range(2):
                ship_q(u, core, k).wait_send()
                out_ship(u, k, core).wait_recv()

        @pl.when((c == last - 1) & shipped(u))
        def _():
            for dev in range(2):
                out_ship(u, dev, k).wait_send()

        @pl.loop(0, chips)
        def _(d):
            @pl.when(to_right(u, d))
            def _():
                for part in range(2):
                    right_copy(u, c - d, part).wait_send()

            @pl.when(to_left(u, d))
            def _():
                left_copy(u, c + d).wait_send()


def on_device(n, queries, stretch_keys, stretch_values, cache_keys, cache_values, prefix_len):
    seqs, rows, width = queries.shape
    pre = cache_keys.shape[1]
    chips = n // 2
    units = HALF * seqs
    keys = n * (pre + rows)
    dma = pltpu.SemaphoreType.DMA
    hbm = pl.BlockSpec(memory_space=pl.ANY)
    vmem = pl.BlockSpec(memory_space=pltpu.VMEM)
    return pl.pallas_call(
        functools.partial(kernel, n),
        out_shape=(
            pltpu.VMEM((seqs, rows, width), jnp.bfloat16),
            pltpu.VMEM((seqs, pre // PAGE, 2 * HK * DH), jnp.bfloat16),
            pltpu.VMEM((seqs, rows // PAGE, 2 * HK * DH), jnp.bfloat16),
        ),
        in_specs=[hbm] * 5 + [pl.BlockSpec(memory_space=pltpu.SMEM)],
        out_specs=(vmem, vmem, vmem),
        scratch_shapes=[
            pltpu.VMEM((HALF, 2, seqs, keys, DH), jnp.bfloat16),
            pltpu.VMEM((2, HALF, seqs, 2, rows, WIDE), jnp.bfloat16),
            pltpu.VMEM((2, HALF, seqs, 2, rows, WIDE), jnp.bfloat16),
            pltpu.VMEM((2, seqs, 2, rows, keys), jnp.float32),
            pltpu.VMEM((seqs, pre, HK * DH), jnp.bfloat16),
            pltpu.VMEM((seqs, rows, HK * DH), jnp.bfloat16),
            dma((units,)),
            dma((units, 4)),
            dma((units, 4)), dma((units, 4)),
            dma((units,)), dma((units,)),
            dma((units, chips, 2)), dma((units, chips, 2)),
            dma((units, chips)), dma((units, chips)),
            dma((units, 2)), dma((units, 2)),
            dma((units,)), dma((units,)),
            dma((units,)),
            dma((units,)), dma((units,)),
            dma((units, 2)), dma((units, 2)),
            dma((2,)),
        ],
        compiler_params=pltpu.CompilerParams(
            collective_id=0, has_side_effects=True, vmem_limit_bytes=60 * 1024 * 1024),
    )(queries, stretch_keys, stretch_values, cache_keys, cache_values, prefix_len)


def solution(mesh):
    rows = P("grp", "seq", None)
    return jax.shard_map(
        functools.partial(on_device, mesh.shape["seq"]),
        mesh=mesh,
        in_specs=(rows, rows, rows, rows, rows, P("grp")),
        out_specs=(rows, rows, rows),
        check_vma=False,
    )
```
